32 devices in a mesh: gx: 4 (over z), gy: 8 (over y, x, core).
Axes of the slice: x: 2, y: 2, z: 4, core: 2. Of those that a mesh axis runs over, the one named last changes fastest.
Arguments:
- atm_members: float32 [4, 8, 80, 12, 128], P('gx', 'gy'), may hold values from -6 to 6
- ocean_members: bfloat16 [4, 8, 80, 1024], P('gx', 'gy'), may hold values from -6 to 6
- remap_weights: bfloat16 [4, 8, 4, 1024, 128], P('gx', 'gy'), may hold values from -0.09375 to 0.09375
- pair_src: int32 [4, 8, 4], P('gx', 'gy'), may hold values from 0 to 31, as said below
- obs_cell: int32 [4, 8, 64], P('gx', 'gy'), may hold values from 0 to 127
- obs_value: float32 [4, 8, 64], P('gx', 'gy'), may hold values from -8 to 8
- obs_error: float32 [4, 8, 64], P('gx', 'gy'), may hold values from 2 to 16
- obs_live: int32 [4, 8, 64], P('gx', 'gy'), may hold values from 0 to 1, as said below
- obs_order: int32 [4, 8, 64], P('gx', 'gy'), may hold values from 0 to 63, each once within a row
Outputs:
- post_mean: float32 [4, 8, 13, 128], P('gx', 'gy')
- post_anom: float32 [4, 8, 80, 13, 128], P('gx', 'gy')
The draws below stay inside these ranges and needn't reach their ends.
Inputs may be any that keep to these rules, and one draw needn't show every extreme that they name: `pair_src`: for atmosphere tile (i, j) the 4 numbers are distinct, each a * 8 + b with |a - i| <= 1 and |b - j| <= 1. `obs_live`: the live slots of a tile are its first ones, between 8 and 64 of them; some tile has all slots live. `obs_order`: each tile's last dimension is a permutation of its slots.
All inputs are finite; a program needn't handle non-finite values.
Results may differ from the reference program's by a relative error of at most 0.0003.
Values may be sent and summed in bfloat16 or wider, within the bound.
A program may use at most 64 MiB of HBM per device.

```python
import math
import jax
import jax.numpy as jnp
from jax import lax

MEM = 80
AX = 8
AY = 16
OCN_DEV = 1024
OB = 32
NB = 2
K = 4
FIELDS = 12
COMP = 13
CELLS = 128
RAD = 2
OBS_DEV = 64
TILES_X = 4
TILES_Y = 8


def draw_pair_src(key, part):
    tile_x = jnp.arange(TILES_X, dtype=jnp.int32)[:, None, None]
    tile_y = jnp.arange(TILES_Y, dtype=jnp.int32)[None, :, None]
    candidate = jnp.arange(9, dtype=jnp.int32)[None, None, :]
    source_x = tile_x + candidate // 3 - 1
    source_y = tile_y + candidate % 3 - 1
    scores = jax.random.randint(jax.random.fold_in(key, 11), (TILES_X, TILES_Y, 9), 0, 1 << 20)
    scores = scores * 9 + candidate
    outside = (source_x < 0) | (source_x >= TILES_X) | (source_y < 0) | (source_y >= TILES_Y)
    scores = jnp.where(outside, scores + (1 << 29), scores)
    ranking = jnp.argsort(scores, axis=-1)[..., :K]
    linear = source_x * TILES_Y + source_y
    return jnp.take_along_axis(linear, ranking, axis=-1).astype(jnp.int32)


def draw_obs_live(key, part):
    threshold = jax.random.randint(jax.random.fold_in(key, 21), (TILES_X, TILES_Y), OBS_DEV // 8, OBS_DEV + 1)
    chosen_tile = jax.random.randint(jax.random.fold_in(key, 22), (), 0, TILES_X * TILES_Y)
    tile_number = jnp.arange(TILES_X * TILES_Y, dtype=jnp.int32).reshape(TILES_X, TILES_Y)
    threshold = jnp.where(tile_number == chosen_tile, OBS_DEV, threshold)
    slot_number = jnp.arange(OBS_DEV, dtype=jnp.int32)
    return (slot_number[None, None, :] < threshold[:, :, None]).astype(jnp.int32)


def plant(values, rng, smallest, top_value):
    longest = values.shape.index(max(values.shape))
    spots = []
    for shift in (0, 1):
        where = [jax.random.randint(jax.random.fold_in(rng, axis), (), 0, length) for axis, length in enumerate(values.shape)]
        where[longest] = (where[longest] + shift) % values.shape[longest]
        spots.append(tuple(where))
    return values.at[spots[0]].set(smallest).at[spots[1]].set(top_value)


def levels(key, shape, pieces, smallest, high):
    level, own = 1.0, jax.random.fold_in(key, 6)
    for axis_at, shards_of in pieces:
        heights = jnp.exp(jax.random.uniform(jax.random.fold_in(own, axis_at), (shards_of,), jnp.float32, smallest / len(pieces), high / len(pieces)))
        level = level * jnp.repeat(heights, shape[axis_at] // shards_of).reshape([-1 if axis == axis_at else 1 for axis in range(len(shape))])
    return level


def centred(rng, shape, spread, limit, pieces=(), held_as=jnp.bfloat16):
    values = spread * jax.random.normal(rng, shape, jnp.float32)
    if pieces:
        values = values * levels(rng, shape, pieces, -0.22, 0.18)
    return jnp.clip(values, -limit, limit).astype(held_as)


def setup_inputs(seed: int = 0) -> dict:
    splits = jax.random.split(jax.random.key(seed), 10)
    atm_members = centred(splits[0], (TILES_X, TILES_Y, MEM, FIELDS, CELLS), 1.0, 6.0, ((0, 4), (1, 8)), jnp.float32)
    ocean_members = centred(splits[1], (TILES_X, TILES_Y, MEM, OCN_DEV), 1.0, 6.0, ((0, 4), (1, 8)))
    remap_weights = centred(splits[2], (TILES_X, TILES_Y, K, OCN_DEV, CELLS), (K * OCN_DEV) ** -0.5, 0.09375, ((0, 4), (1, 8)))
    pair_src = draw_pair_src(jax.random.fold_in(splits[9], 71), 0)
    obs_cell = plant(jax.random.randint(splits[4], (TILES_X, TILES_Y, OBS_DEV), 0, CELLS), jax.random.fold_in(splits[4], 1), 0, CELLS - 1).astype(jnp.int32)
    obs_value = centred(splits[5], (TILES_X, TILES_Y, OBS_DEV), 1.5, 8.0, ((0, 4), (1, 8)), jnp.float32)
    obs_error = jnp.clip(jnp.exp(math.log(16.0) - 2.0794415 * jax.random.uniform(splits[6], (TILES_X, TILES_Y, OBS_DEV), jnp.float32) ** levels(splits[6], (TILES_X, TILES_Y, OBS_DEV), ((0, 4), (1, 8)), -0.2, 0.2)), 2.0, 16.0)
    obs_live = draw_obs_live(jax.random.fold_in(splits[9], 71), 0)
    obs_order = jax.vmap(lambda own: jax.random.permutation(own, OBS_DEV))(jax.random.split(splits[8], TILES_X * TILES_Y)).reshape((TILES_X, TILES_Y, OBS_DEV)).astype(jnp.int32)
    return {"atm_members": atm_members, "ocean_members": ocean_members, "remap_weights": remap_weights, "pair_src": pair_src, "obs_cell": obs_cell, "obs_value": obs_value, "obs_error": obs_error, "obs_live": obs_live, "obs_order": obs_order}


exact_mode = lax.Precision.HIGHEST

def update_group(packets, anomaly, ens_mean, base_x, base_y):
    members = anomaly.shape[0]
    components = anomaly.shape[1]
    cell_count = anomaly.shape[2]
    observed = jnp.transpose(packets[:, :members, :], (1, 0, 2)).reshape(members, -1)
    innovation = packets[:, members, :].reshape(-1)
    errors = packets[:, members + 1, :].reshape(-1)
    obs_x = packets[:, members + 2, :].reshape(-1)
    obs_y = packets[:, members + 3, :].reshape(-1)
    live = packets[:, members + 4, :].reshape(-1)
    variance = lax.optimization_barrier(jnp.sum(observed * observed, axis=0)) / (members - 1)
    denominator = variance + errors + (1.0 - live)
    weighting = live / denominator
    damping = 1.0 / (1.0 + jnp.sqrt(errors / denominator))
    cell_index = jnp.arange(cell_count, dtype=jnp.int32)
    cell_x = (base_x + cell_index // AY).astype(jnp.float32)
    cell_y = (base_y + cell_index % AY).astype(jnp.float32)
    distance = (obs_x[:, None] - cell_x[None, :]) ** 2 + (obs_y[:, None] - cell_y[None, :]) ** 2
    taper = jnp.maximum(1.0 - distance / float(RAD * RAD), 0.0) ** 2
    flat_anomaly = anomaly.reshape(members, components * cell_count)
    covariance = jnp.dot(observed.T, flat_anomaly, precision=exact_mode, preferred_element_type=jnp.float32) / (members - 1)
    gain = covariance.reshape(-1, components, cell_count) * (taper * weighting[:, None])[:, None, :]
    gain = gain.reshape(-1, components * cell_count)
    mean_step = jnp.dot(innovation[None, :], gain, precision=exact_mode, preferred_element_type=jnp.float32)
    anomaly_step = jnp.dot(observed * damping[None, :], gain, precision=exact_mode, preferred_element_type=jnp.float32)
    return (mean_step.reshape(components, cell_count), anomaly_step.reshape(members, components, cell_count))

def reference(atm_members, ocean_members, remap_weights, pair_src, obs_cell, obs_value, obs_error, obs_live, obs_order):
    tiles = TILES_X * TILES_Y
    ocean_flat = ocean_members.reshape(tiles, MEM, OCN_DEV)

    def remap_one(inputs):
        weights, sources = inputs
        chosen = ocean_flat[sources]
        stacked = jnp.transpose(chosen, (1, 0, 2)).reshape(MEM, K * OCN_DEV)
        return jnp.dot(stacked, weights.reshape(K * OCN_DEV, CELLS), preferred_element_type=jnp.float32)
    surface = lax.map(remap_one, (remap_weights.reshape(tiles, K, OCN_DEV, CELLS), pair_src.reshape(tiles, K).astype(jnp.int32)))
    state = jnp.concatenate([atm_members.reshape(tiles, MEM, FIELDS, CELLS), surface[:, :, None, :]], axis=2)
    ens_mean = lax.optimization_barrier(jnp.sum(state, axis=1)) / MEM
    anomaly = state - ens_mean[:, None]
    ens_mean = ens_mean.reshape(TILES_X, TILES_Y, COMP, CELLS)
    anomaly = anomaly.reshape(TILES_X, TILES_Y, MEM, COMP, CELLS)
    tile_x = jnp.broadcast_to(jnp.arange(TILES_X, dtype=jnp.int32)[:, None], (TILES_X, TILES_Y))
    tile_y = jnp.broadcast_to(jnp.arange(TILES_Y, dtype=jnp.int32)[None, :], (TILES_X, TILES_Y))
    base_x = tile_x * AX
    base_y = tile_y * AY
    for batch_index in range(NB):
        obs_slots = obs_order[:, :, batch_index * OB:(batch_index + 1) * OB].astype(jnp.int32)
        obs_cells = jnp.take_along_axis(obs_cell.astype(jnp.int32), obs_slots, axis=2)
        values = jnp.take_along_axis(obs_value, obs_slots, axis=2)
        errors = jnp.take_along_axis(obs_error, obs_slots, axis=2)
        live = jnp.take_along_axis(obs_live, obs_slots, axis=2).astype(jnp.float32)
        observed = jnp.take_along_axis(anomaly[:, :, :, FIELDS, :], obs_cells[:, :, None, :], axis=3)
        predicted = jnp.take_along_axis(ens_mean[:, :, FIELDS, :], obs_cells, axis=2)
        pos_x = (base_x[:, :, None] + obs_cells // AY).astype(jnp.float32)
        pos_y = (base_y[:, :, None] + obs_cells % AY).astype(jnp.float32)
        extras = jnp.stack([values - predicted, errors, pos_x, pos_y, live], axis=2)
        packet = jnp.concatenate([observed, extras], axis=2)
        padded = jnp.pad(packet, ((1, 1), (1, 1), (0, 0), (0, 0)))
        beside_all = jnp.stack([padded[row_shift:row_shift + TILES_X, col_shift:col_shift + TILES_Y] for row_shift in range(3) for col_shift in range(3)], axis=2)

        def one_tile(inputs):
            packets, tile_anomaly, tile_mean, anchor_x, anchor_y = inputs
            mean_step, anomaly_step = update_group(packets, tile_anomaly, tile_mean, anchor_x, anchor_y)
            return (tile_mean + mean_step, tile_anomaly - anomaly_step)
        new_mean, new_anomaly = lax.map(one_tile, (beside_all.reshape(tiles, 9, MEM + 5, OB), anomaly.reshape(tiles, MEM, COMP, CELLS), ens_mean.reshape(tiles, COMP, CELLS), base_x.reshape(tiles), base_y.reshape(tiles)))
        ens_mean = new_mean.reshape(TILES_X, TILES_Y, COMP, CELLS)
        anomaly = new_anomaly.reshape(TILES_X, TILES_Y, MEM, COMP, CELLS)
    return (ens_mean, anomaly)
```

```python
import functools

import jax
import jax.numpy as jnp
import numpy as np
from jax import lax
from jax.experimental import pallas as pl
from jax.experimental.pallas import tpu as pltpu
from jax.sharding import PartitionSpec as P

AX = 8
AY = 16
OB = 32
NB = 2
RAD = 2
CODE = 64

MESH = pl.DeviceIdType.MESH
OFFS = [(dx, dy) for dx in (-1, 0, 1) for dy in (-1, 0, 1)]
OTHERS = [i for i in range(9) if i != 4]


def taper_of(dx, dy):
    return max(1.0 - (dx * dx + dy * dy) / float(RAD * RAD), 0.0) ** 2


@functools.lru_cache
def tables():
    cells = AX * AY
    own = [(c // AY, c % AY) for c in range(cells)]
    halo = [
        (x, y)
        for x in range(-RAD, AX + RAD)
        for y in range(-RAD, AY + RAD)
        if not (0 <= x < AX and 0 <= y < AY)
    ]
    lanes = own + halo
    where = {xy: n for n, xy in enumerate(lanes)}
    code = np.full((8, 2 * cells), -1.0, np.float32)
    for n, (x, y) in enumerate(lanes):
        code[:, n] = (x + AX) * CODE + (y + AY)
    move = np.zeros((2 * cells, 2, 8, cells), np.float32)
    for n, (x, y) in enumerate(lanes):
        for d, i in enumerate(OTHERS):
            dx, dy = OFFS[i]
            src = where.get((x + dx, y + dy))
            if src is not None:
                move[src, n // cells, d, n % cells] = 1.0
    pick = np.zeros((8, cells, cells), np.float32)
    for n, (x, y) in enumerate(halo):
        i = (x // AX + 1) * 3 + (y // AY + 1)
        pick[OTHERS.index(i), (x % AX) * AY + (y % AY), n] = 1.0
    return code, move.reshape(2 * cells, 16 * cells), pick.reshape(8 * cells, cells)


def exchange_kernel(
    src_ref, meta_ref, ocean_ref, weights_ref, atm_ref,
    tiles_ref, metat_ref, fields_ref, fmean_ref,
    ocn, wts, meta, local_sem, send_sem, recv_sem,
):
    gx, gy = lax.axis_index("gx"), lax.axis_index("gy")
    nx, ny = lax.axis_size("gx"), lax.axis_size("gy")
    members = tiles_ref.shape[1]
    fields = fields_ref.shape[0]

    def there(i):
        dx, dy = OFFS[i]
        return (gx + dx >= 0) & (gx + dx < nx) & (gy + dy >= 0) & (gy + dy < ny)

    own_in = pltpu.make_async_copy(ocean_ref, ocn.at[4], local_sem.at[0])
    own_in.start()
    w_in = pltpu.make_async_copy(weights_ref, wts, local_sem.at[1])
    w_in.start()
    atm_in = pltpu.make_async_copy(atm_ref, fields_ref, local_sem.at[2])
    atm_in.start()

    barrier = pltpu.get_barrier_semaphore()
    for i in OTHERS:
        dx, dy = OFFS[i]

        @pl.when(there(i))
        def _():
            pl.semaphore_signal(barrier, inc=1, device_id=(gx + dx, gy + dy), device_id_type=MESH)

    rows = meta_ref[...]
    order = rows[0:1, :]
    slot = lax.broadcasted_iota(jnp.int32, (rows.shape[1], rows.shape[1]), 0).astype(jnp.float32)
    perm = jnp.where(order == slot, 1.0, 0.0)
    meta[4] = jnp.dot(
        rows, perm, precision=lax.Precision.HIGHEST, preferred_element_type=jnp.float32
    )
    for n in range(9, meta.shape[0]):
        meta[n] = jnp.zeros(meta.shape[1:], jnp.float32)
    across = 1 + (gx > 0).astype(jnp.int32) + (gx < nx - 1).astype(jnp.int32)
    along = 1 + (gy > 0).astype(jnp.int32) + (gy < ny - 1).astype(jnp.int32)
    pl.semaphore_wait(barrier, across * along - 1)
    for i in OTHERS:

        @pl.when(jnp.logical_not(there(i)))
        def _():
            tiles_ref[i] = jnp.zeros(tiles_ref.shape[1:], jnp.float32)
            meta[i] = jnp.zeros(meta.shape[1:], jnp.float32)

    own_in.wait()

    def remote(buf, kind, i):
        dx, dy = OFFS[i]
        return pltpu.make_async_remote_copy(
            src_ref=buf.at[4],
            dst_ref=buf.at[8 - i],
            send_sem=send_sem.at[kind, i],
            recv_sem=recv_sem.at[kind, 8 - i],
            device_id=(gx + dx, gy + dy),
            device_id_type=MESH,
        )

    def arrival(buf, kind, i):
        return pltpu.make_async_remote_copy(
            src_ref=buf.at[4],
            dst_ref=buf.at[i],
            send_sem=send_sem.at[kind, i],
            recv_sem=recv_sem.at[kind, i],
            device_id=(gx + OFFS[i][0], gy + OFFS[i][1]),
            device_id_type=MESH,
        )

    def send(buf, kind):
        for i in OTHERS:

            @pl.when(there(i))
            def _():
                remote(buf, kind, i).start()

    def receive(buf, kind):
        for i in OTHERS:

            @pl.when(there(i))
            def _():
                arrival(buf, kind, i).wait_recv()

    def settle(buf, kind):
        for i in OTHERS:

            @pl.when(there(i))
            def _():
                remote(buf, kind, i).wait_send()

    send(ocn, 0)
    send(meta, 1)

    atm_in.wait()
    for v in range(fields):
        block = fields_ref[v]
        mean = jnp.sum(block, axis=0, keepdims=True) / members
        fmean_ref[v : v + 1, :] = mean
        fields_ref[v] = block - mean
    receive(meta, 1)
    flat = meta[...].reshape(meta.shape[0] * meta.shape[1], meta.shape[2])
    metat_ref[...] = flat.T
    w_in.wait()
    receive(ocn, 0)
    total = jnp.zeros(tiles_ref.shape[1:], jnp.float32)
    for k in range(wts.shape[0]):
        source = src_ref[k]
        position = (source // ny - gx + 1) * 3 + (source % ny - gy + 1)
        position = jnp.clip(position, 0, 8)
        total += jnp.dot(ocn[position], wts[k], preferred_element_type=jnp.float32)
    tiles_ref[4] = total
    send(tiles_ref, 2)
    settle(ocn, 0)
    settle(meta, 1)
    receive(tiles_ref, 2)
    settle(tiles_ref, 2)


def split_rows(block):
    high = block.astype(jnp.bfloat16).astype(jnp.float32)
    return jnp.concatenate([high, block - high], axis=0).astype(jnp.bfloat16)


def analysis_kernel(
    tiles_ref, metat_ref, fields_ref, fmean_ref, code_ref, move_ref, pick_ref,
    mean_ref, anom_ref,
    held, shifted, out_sem,
):
    fields, members, cells = fields_ref.shape
    scale = 1.0 / (members - 1)
    beside = split_rows(jnp.concatenate([tiles_ref[i] for i in OTHERS], axis=1))
    halo = jnp.dot(beside, pick_ref[...], preferred_element_type=jnp.float32)
    grid = jnp.concatenate([tiles_ref[4], halo[:members] + halo[members:]], axis=1)
    gmean = jnp.sum(grid, axis=0, keepdims=True) / members
    grid = grid - gmean
    code = code_ref[0:1, :]

    for b in range(NB):
        last = b == NB - 1
        variance = jnp.sum(grid * grid, axis=0, keepdims=True) / (members - 1)
        gains = jnp.zeros((OB, 2 * cells), jnp.float32)
        sums = jnp.zeros((OB, 2 * cells), jnp.float32)
        weights = jnp.zeros((OB, 2 * cells), jnp.float32)
        for i in range(9):
            dx, dy = OFFS[i]
            column = metat_ref[b * OB : (b + 1) * OB, 8 * i : 8 * i + 8]
            spot = column[:, 1:2] + float((AX * dx + AX) * CODE + AY * dy + AY)
            error = column[:, 3:4]
            live = column[:, 4:5]
            denom = variance + (error + (1.0 - live))
            weighting = live / denom
            damping = 1.0 / (1.0 + jnp.sqrt(error / denom))
            hit = spot == code
            weighting = jnp.where(hit, weighting, 0.0)
            weights = weights + weighting
            gains = gains + weighting * damping
            sums = sums + weighting * column[:, 2:3]
        alpha = jnp.sum(gains, axis=0, keepdims=True)
        beta = jnp.sum(sums, axis=0, keepdims=True) - gmean * jnp.sum(weights, axis=0, keepdims=True)
        extra = jnp.concatenate([alpha, beta, jnp.zeros((6, 2 * cells), jnp.float32)], axis=0)
        left = split_rows(jnp.concatenate([grid, extra], axis=0))
        width = (8 if last else 16) * cells
        moved = jnp.dot(left, move_ref[:, :width], preferred_element_type=jnp.float32)
        rows = members + 8
        shifted[:, :width] = moved[:rows] + moved[rows:]

        def step(block, part, center, alpha, beta):
            total = jnp.zeros_like(block)
            mean = jnp.zeros((1, cells), jnp.float32)
            for d in range(9):
                if d == 8:
                    source, a, m = center, alpha * scale, beta * scale
                else:
                    dx, dy = OFFS[OTHERS[d]]
                    weight = scale * taper_of(dx, dy)
                    at = (part * 8 + d) * cells
                    source = shifted[:members, at : at + cells]
                    a = shifted[members : members + 1, at : at + cells] * weight
                    m = shifted[members + 1 : members + 2, at : at + cells] * weight
                cov = jnp.sum(block * source, axis=0, keepdims=True)
                mean = mean + cov * m
                total = total + source * (cov * a)
            return block - total, mean

        own = grid[:, :cells]
        held[fields] = own
        own_args = (alpha[:, :cells], beta[:, :cells])
        origin = fields_ref if b == 0 else held

        def one_field(v, carry, origin=origin, own_args=own_args, last=last, b=b, step=step):
            block, mean = step(origin[v], 0, held[fields], *own_args)
            held[v] = block
            before = fmean_ref[pl.ds(v, 1), :] if b == 0 else mean_ref[pl.ds(v, 1), :]
            mean_ref[pl.ds(v, 1), :] = before + mean
            if last:
                pltpu.make_async_copy(held.at[v], anom_ref.at[v], out_sem.at[v]).start()
            return carry

        lax.fori_loop(0, fields, one_field, 0)
        block, mean = step(own, 0, own, *own_args)
        if last:
            held[fields] = block
            mean_ref[fields : fields + 1, :] = gmean[:, :cells] + mean
            pltpu.make_async_copy(
                held.at[fields], anom_ref.at[fields], out_sem.at[fields]
            ).start()
            for v in range(fields + 1):
                pltpu.make_async_copy(held.at[v], anom_ref.at[v], out_sem.at[v]).wait()
        else:
            outer = grid[:, cells:]
            far, far_mean = step(outer, 1, outer, alpha[:, cells:], beta[:, cells:])
            grid = jnp.concatenate([block, far], axis=1)
            gmean = gmean + jnp.concatenate([mean, far_mean], axis=1)


def local(
    atm_members, ocean_members, remap_weights, pair_src, obs_cell, obs_value, obs_error,
    obs_live, obs_order,
):
    members, fields, cells = atm_members.shape[2:]
    slots = obs_cell.shape[2]
    sources, depth = remap_weights.shape[2:4]
    cell = obs_cell[0, 0]
    spot = ((cell // AY) * CODE + cell % AY).astype(jnp.float32)
    meta = jnp.stack(
        [
            obs_order[0, 0].astype(jnp.float32), spot, obs_value[0, 0], obs_error[0, 0],
            obs_live[0, 0].astype(jnp.float32),
        ]
    )
    meta = jnp.pad(meta, ((0, 3), (0, cells - slots)))
    vmem = pl.BlockSpec(memory_space=pltpu.VMEM)
    hbm = pl.BlockSpec(memory_space=pltpu.HBM)
    tiles, metat, anomalies, fmean = pl.pallas_call(
        exchange_kernel,
        out_shape=(
            jax.ShapeDtypeStruct((9, members, cells), jnp.float32),
            jax.ShapeDtypeStruct((128, 128), jnp.float32),
            jax.ShapeDtypeStruct((fields, members, cells), jnp.float32),
            jax.ShapeDtypeStruct((fields, cells), jnp.float32),
        ),
        in_specs=[pl.BlockSpec(memory_space=pltpu.SMEM), vmem, hbm, hbm, hbm],
        out_specs=(vmem,) * 4,
        scratch_shapes=[
            pltpu.VMEM((9, members, depth), jnp.bfloat16),
            pltpu.VMEM((sources, depth, cells), jnp.bfloat16),
            pltpu.VMEM((16, 8, 128), jnp.float32),
            pltpu.SemaphoreType.DMA((3,)),
            pltpu.SemaphoreType.DMA((3, 9)),
            pltpu.SemaphoreType.DMA((3, 9)),
        ],
        compiler_params=pltpu.CompilerParams(
            collective_id=0, has_side_effects=True, vmem_limit_bytes=16 << 20
        ),
        name="exchange",
    )(pair_src[0, 0], meta, ocean_members[0, 0], remap_weights[0, 0],
        jnp.transpose(atm_members[0, 0], (1, 0, 2)))
    code, move, pick = tables()
    post_mean, post_anom = pl.pallas_call(
        analysis_kernel,
        out_shape=(
            jax.ShapeDtypeStruct((fields + 1, cells), jnp.float32),
            jax.ShapeDtypeStruct((fields + 1, members, cells), jnp.float32),
        ),
        in_specs=[vmem] * 7,
        out_specs=(vmem, hbm),
        scratch_shapes=[
            pltpu.VMEM((fields + 1, members, cells), jnp.float32),
            pltpu.VMEM((members + 8, 16 * cells), jnp.float32),
            pltpu.SemaphoreType.DMA((fields + 1,)),
        ],
        compiler_params=pltpu.CompilerParams(vmem_limit_bytes=24 << 20),
        name="analysis",
    )(
        tiles, metat, anomalies, fmean, jnp.asarray(code),
        jnp.asarray(move, jnp.bfloat16), jnp.asarray(pick, jnp.bfloat16),
    )
    return (post_mean[None, None], jnp.transpose(post_anom, (1, 0, 2))[None, None])


def solution(mesh):
    in_specs = (
        P("gx", "gy", None, None, None),
        P("gx", "gy", None, None),
        P("gx", "gy", None, None, None),
        P("gx", "gy", None),
        P("gx", "gy", None),
        P("gx", "gy", None),
        P("gx", "gy", None),
        P("gx", "gy", None),
        P("gx", "gy", None),
    )
    out_specs = (P("gx", "gy", None, None), P("gx", "gy", None, None, None))
    return jax.shard_map(local, mesh=mesh, in_specs=in_specs, out_specs=out_specs, check_vma=False)
```

```python
import functools

import jax
import jax.numpy as jnp
import numpy as np
from jax import lax
from jax.experimental import pallas as pl
from jax.experimental.pallas import tpu as pltpu
from jax.sharding import PartitionSpec as P

AX = 8
AY = 16
OB = 32
NB = 2
RAD = 2
CODE = 64
LIMIT = 66977792

MESH = pl.DeviceIdType.MESH
OFFS = [(dx, dy) for dx in (-1, 0, 1) for dy in (-1, 0, 1)]
OTHERS = [i for i in range(9) if i != 4]


def taper_of(dx, dy):
    return max(1.0 - (dx * dx + dy * dy) / float(RAD * RAD), 0.0) ** 2


@functools.lru_cache
def tables():
    cells = AX * AY
    own = [(c // AY, c % AY) for c in range(cells)]
    halo = [
        (x, y)
        for x in range(-RAD, AX + RAD)
        for y in range(-RAD, AY + RAD)
        if not (0 <= x < AX and 0 <= y < AY)
    ]
    lanes = own + halo
    where = {xy: n for n, xy in enumerate(lanes)}
    code = np.full((8, 2 * cells), -1.0, np.float32)
    for n, (x, y) in enumerate(lanes):
        code[:, n] = (x + AX) * CODE + (y + AY)
    move = np.zeros((2 * cells, 2, 8, cells), np.float32)
    for n, (x, y) in enumerate(lanes):
        for d, i in enumerate(OTHERS):
            dx, dy = OFFS[i]
            src = where.get((x + dx, y + dy))
            if src is not None:
                move[src, n // cells, d, n % cells] = 1.0
    pick = np.zeros((8, cells, cells), np.float32)
    for n, (x, y) in enumerate(halo):
        i = (x // AX + 1) * 3 + (y // AY + 1)
        pick[OTHERS.index(i), (x % AX) * AY + (y % AY), n] = 1.0
    return code, move.reshape(2 * cells, 16 * cells), pick.reshape(8 * cells, cells)


def split_rows(block):
    high = block.astype(jnp.bfloat16).astype(jnp.float32)
    return jnp.concatenate([high, block - high], axis=0).astype(jnp.bfloat16)


def kernel(
    src_ref, order_ref, cell_ref, live_ref, value_ref, error_ref, ocean_ref, weights_ref, atm_ref,
    code_in, move_in, pick_in,
    mean_ref, anom_ref,
    ocn, wts, meta, src, order_in, cell_in, live_in, value_in, error_in,
    tiles_ref, metat_ref, code_ref, move_ref, pick_ref, held, shifted,
    local_sem, send_sem, recv_sem, out_sem,
):
    gx, gy = lax.axis_index("gx"), lax.axis_index("gy")
    nx, ny = lax.axis_size("gx"), lax.axis_size("gy")
    members = tiles_ref.shape[1]
    fields = atm_ref.shape[0]
    cells = tiles_ref.shape[2]
    slots = order_in.shape[1]

    def has_x(dx):
        return (gx + dx >= 0) & (gx + dx < nx)

    def has_y(dy):
        return (gy + dy >= 0) & (gy + dy < ny)

    def there(i):
        return has_x(OFFS[i][0]) & has_y(OFFS[i][1])

    pairs = (
        (ocean_ref, ocn.at[4]), (order_ref, order_in), (cell_ref, cell_in), (live_ref, live_in),
        (value_ref, value_in), (error_ref, error_in), (src_ref, src), (weights_ref, wts),
        (atm_ref, held.at[0:fields]), (code_in, code_ref), (move_in, move_ref), (pick_in, pick_ref),
    )
    staged = [pltpu.make_async_copy(x, y, local_sem.at[n]) for n, (x, y) in enumerate(pairs)]
    for copy in staged:
        copy.start()

    barrier = pltpu.get_barrier_semaphore()
    for i in OTHERS:
        dx, dy = OFFS[i]

        @pl.when(there(i))
        def _():
            pl.semaphore_signal(barrier, inc=1, device_id=(gx + dx, gy + dy), device_id_type=MESH)

    for i in OTHERS:

        @pl.when(jnp.logical_not(there(i)))
        def _():
            tiles_ref[i] = jnp.zeros(tiles_ref.shape[1:], jnp.float32)
            meta[i] = jnp.zeros(meta.shape[1:], jnp.float32)

    for n in range(9, meta.shape[0]):
        meta[n] = jnp.zeros(meta.shape[1:], jnp.float32)

    for copy in staged[1:6]:
        copy.wait()
    cell = cell_in[...]
    spot = ((cell // AY) * CODE + cell % AY).astype(jnp.float32)
    rows = jnp.concatenate(
        [
            spot, value_in[...], error_in[...], live_in[...].astype(jnp.float32),
            jnp.zeros((4, slots), jnp.float32),
        ],
        axis=0,
    )
    slot = lax.broadcasted_iota(jnp.int32, (slots, slots), 0)
    perm = jnp.where(order_in[...] == slot, 1.0, 0.0)
    rows = jnp.dot(rows, perm, precision=lax.Precision.HIGHEST, preferred_element_type=jnp.float32)
    meta[4] = jnp.concatenate([rows, jnp.zeros((8, meta.shape[2] - slots), jnp.float32)], axis=1)

    staged[0].wait()
    across = 1 + has_x(-1).astype(jnp.int32) + has_x(1).astype(jnp.int32)
    along = 1 + has_y(-1).astype(jnp.int32) + has_y(1).astype(jnp.int32)
    pl.semaphore_wait(barrier, across * along - 1)

    outer = lax.rem(gy, 2) * 2 - 1

    def ocean(source, target, n, dx, dy):
        return pltpu.make_async_remote_copy(
            src_ref=ocn.at[source],
            dst_ref=ocn.at[target],
            send_sem=send_sem.at[0, n],
            recv_sem=recv_sem.at[0, target],
            device_id=(gx + dx, gy + dy),
            device_id_type=MESH,
        )

    def arrive(at, dx, dy):
        ocean(at, at, 4, dx, dy).wait_recv()

    firsts = [
        (has_y(outer), ocean(4, 4 - outer, 1, 0, outer)),
        (has_x(-1), ocean(4, 7, 2, -1, 0)),
        (has_x(1), ocean(4, 1, 3, 1, 0)),
        (has_y(-outer), ocean(4, 4 + outer, 0, 0, -outer)),
    ]
    relays = [
        (has_y(outer) & has_x(dx), ocean(4 + outer, 4 - 3 * dx + outer, n, dx, 0))
        for dx, n in ((-1, 5), (1, 6))
    ]
    hands = [
        (dx, has_x(dx) & has_y(-outer), ocean(4 + 3 * dx, 4 + 3 * dx + outer, n, 0, -outer))
        for dx, n in ((-1, 7), (1, 8))
    ]

    def begin(cond, copy):
        @pl.when(cond)
        def _():
            copy.start()

    for cond, copy in firsts:
        begin(cond, copy)

    def remote(buf, kind, i):
        dx, dy = OFFS[i]
        return pltpu.make_async_remote_copy(
            src_ref=buf.at[4],
            dst_ref=buf.at[8 - i],
            send_sem=send_sem.at[kind, i],
            recv_sem=recv_sem.at[kind, 8 - i],
            device_id=(gx + dx, gy + dy),
            device_id_type=MESH,
        )

    def send(buf, kind):
        for i in OTHERS:

            @pl.when(there(i))
            def _():
                remote(buf, kind, i).start()

    def receive(buf, kind):
        for i in OTHERS:

            @pl.when(there(i))
            def _():
                remote(buf, kind, 8 - i).wait_recv()

    def settle(buf, kind):
        for i in OTHERS:

            @pl.when(there(i))
            def _():
                remote(buf, kind, i).wait_send()

    send(meta, 1)

    staged[8].wait()
    for v in range(fields):
        block = held[v]
        mean = jnp.sum(block, axis=0, keepdims=True) / members
        mean_ref[v] = mean
        held[v] = block - mean

    @pl.when(has_y(outer))
    def _():
        arrive(4 + outer, 0, outer)

    for cond, copy in relays:
        begin(cond, copy)
    for dx, cond, copy in hands:

        @pl.when(has_x(dx))
        def _():
            arrive(4 + 3 * dx, dx, 0)

        begin(cond, copy)

    receive(meta, 1)
    flat = meta[...].reshape(meta.shape[0] * meta.shape[1], meta.shape[2])
    metat_ref[...] = flat.T
    staged[6].wait()
    staged[7].wait()
    for copy in staged[9:]:
        copy.wait()

    @pl.when(has_y(-outer))
    def _():
        arrive(4 - outer, 0, -outer)

    for dx in (-1, 1):
        for dy in (outer, -outer):

            @pl.when(has_x(dx) & has_y(dy))
            def _():
                arrive(4 + 3 * dx + dy, dx, 0)

    total = jnp.zeros(tiles_ref.shape[1:], jnp.float32)
    for k in range(wts.shape[0]):
        source = src[0, k]
        position = (source // ny - gx + 1) * 3 + (source % ny - gy + 1)
        position = jnp.clip(position, 0, 8)
        total += jnp.dot(ocn[position], wts[k], preferred_element_type=jnp.float32)
    tiles_ref[4] = total
    send(tiles_ref, 2)
    for cond, copy in firsts + relays + [hand[1:] for hand in hands]:

        @pl.when(cond)
        def _():
            copy.wait_send()

    settle(meta, 1)
    receive(tiles_ref, 2)
    settle(tiles_ref, 2)

    scale = 1.0 / (members - 1)
    beside = split_rows(jnp.concatenate([tiles_ref[i] for i in OTHERS], axis=1))
    halo = jnp.dot(beside, pick_ref[...], preferred_element_type=jnp.float32)
    grid = jnp.concatenate([tiles_ref[4], halo[:members] + halo[members:]], axis=1)
    gmean = jnp.sum(grid, axis=0, keepdims=True) / members
    grid = grid - gmean
    code = code_ref[0:1, :]

    for b in range(NB):
        last = b == NB - 1
        variance = jnp.sum(grid * grid, axis=0, keepdims=True) / (members - 1)
        gains = jnp.zeros((OB, 2 * cells), jnp.float32)
        sums = jnp.zeros((OB, 2 * cells), jnp.float32)
        weights = jnp.zeros((OB, 2 * cells), jnp.float32)
        for i in range(9):
            dx, dy = OFFS[i]
            column = metat_ref[b * OB : (b + 1) * OB, 8 * i : 8 * i + 4]
            spot = column[:, 0:1] + float((AX * dx + AX) * CODE + AY * dy + AY)
            error = column[:, 2:3]
            live = column[:, 3:4]
            denom = variance + (error + (1.0 - live))
            weighting = live / denom
            damping = 1.0 / (1.0 + jnp.sqrt(error / denom))
            hit = spot == code
            weighting = jnp.where(hit, weighting, 0.0)
            weights = weights + weighting
            gains = gains + weighting * damping
            sums = sums + weighting * column[:, 1:2]
        alpha = jnp.sum(gains, axis=0, keepdims=True)
        beta = jnp.sum(sums, axis=0, keepdims=True) - gmean * jnp.sum(weights, axis=0, keepdims=True)
        extra = jnp.concatenate([alpha, beta, jnp.zeros((6, 2 * cells), jnp.float32)], axis=0)
        left = split_rows(jnp.concatenate([grid, extra], axis=0))
        width = (8 if last else 16) * cells
        moved = jnp.dot(left, move_ref[:, :width], preferred_element_type=jnp.float32)
        rows = members + 8
        shifted[:, :width] = moved[:rows] + moved[rows:]

        def step(block, part, center, alpha, beta):
            total = jnp.zeros_like(block)
            mean = jnp.zeros((1, cells), jnp.float32)
            for d in range(9):
                if d == 8:
                    source, a, m = center, alpha * scale, beta * scale
                else:
                    dx, dy = OFFS[OTHERS[d]]
                    weight = scale * taper_of(dx, dy)
                    at = (part * 8 + d) * cells
                    source = shifted[:members, at : at + cells]
                    a = shifted[members : members + 1, at : at + cells] * weight
                    m = shifted[members + 1 : members + 2, at : at + cells] * weight
                cov = jnp.sum(block * source, axis=0, keepdims=True)
                mean = mean + cov * m
                total = total + source * (cov * a)
            return block - total, mean

        own = grid[:, :cells]
        held[fields] = own
        own_args = (alpha[:, :cells], beta[:, :cells])

        def one_field(v, carry, own_args=own_args, last=last, step=step):
            block, mean = step(held[v], 0, held[fields], *own_args)
            held[v] = block
            mean_ref[v] = mean_ref[v] + mean
            if last:
                pltpu.make_async_copy(held.at[v], anom_ref.at[v], out_sem.at[v]).start()
            return carry

        lax.fori_loop(0, fields, one_field, 0)
        block, mean = step(own, 0, own, *own_args)
        if last:
            held[fields] = block
            mean_ref[fields] = gmean[:, :cells] + mean
            pltpu.make_async_copy(
                held.at[fields], anom_ref.at[fields], out_sem.at[fields]
            ).start()
            for v in range(fields + 1):
                pltpu.make_async_copy(held.at[v], anom_ref.at[v], out_sem.at[v]).wait()
        else:
            outer = grid[:, cells:]
            far, far_mean = step(outer, 1, outer, alpha[:, cells:], beta[:, cells:])
            grid = jnp.concatenate([block, far], axis=1)
            gmean = gmean + jnp.concatenate([mean, far_mean], axis=1)


def local(
    atm_members, ocean_members, remap_weights, pair_src, obs_cell, obs_value, obs_error,
    obs_live, obs_order,
):
    members, fields, cells = atm_members.shape[2:]
    slots = obs_cell.shape[2]
    sources, depth = remap_weights.shape[2:4]
    vmem = pl.BlockSpec(memory_space=pltpu.VMEM)
    anywhere = pl.BlockSpec(memory_space=pl.ANY)
    code, move, pick = tables()
    post_mean, post_anom = pl.pallas_call(
        kernel,
        out_shape=(
            jax.ShapeDtypeStruct((fields + 1, 1, cells), jnp.float32),
            jax.ShapeDtypeStruct((fields + 1, members, cells), jnp.float32),
        ),
        in_specs=[anywhere] * 12,
        out_specs=(vmem, anywhere),
        scratch_shapes=[
            pltpu.VMEM((9, members, depth), jnp.bfloat16),
            pltpu.VMEM((sources, depth, cells), jnp.bfloat16),
            pltpu.VMEM((16, 8, 128), jnp.float32),
            pltpu.SMEM((1, sources), jnp.int32),
            pltpu.VMEM((1, slots), jnp.int32),
            pltpu.VMEM((1, slots), jnp.int32),
            pltpu.VMEM((1, slots), jnp.int32),
            pltpu.VMEM((1, slots), jnp.float32),
            pltpu.VMEM((1, slots), jnp.float32),
            pltpu.VMEM((9, members, cells), jnp.float32),
            pltpu.VMEM((128, 128), jnp.float32),
            pltpu.VMEM(code.shape, jnp.float32),
            pltpu.VMEM(move.shape, jnp.bfloat16),
            pltpu.VMEM(pick.shape, jnp.bfloat16),
            pltpu.VMEM((fields + 1, members, cells), jnp.float32),
            pltpu.VMEM((members + 8, 16 * cells), jnp.float32),
            pltpu.SemaphoreType.DMA((12,)),
            pltpu.SemaphoreType.DMA((3, 9)),
            pltpu.SemaphoreType.DMA((3, 9)),
            pltpu.SemaphoreType.DMA((fields + 1,)),
        ],
        compiler_params=pltpu.CompilerParams(
            collective_id=0, has_side_effects=True, vmem_limit_bytes=LIMIT
        ),
        name="fused",
    )(
        pair_src[0], obs_order[0], obs_cell[0], obs_live[0], obs_value[0], obs_error[0],
        ocean_members[0, 0], remap_weights[0, 0], jnp.transpose(atm_members[0, 0], (1, 0, 2)),
        jnp.asarray(code), jnp.asarray(move, jnp.bfloat16), jnp.asarray(pick, jnp.bfloat16),
    )
    return (post_mean.reshape(1, 1, fields + 1, cells), jnp.transpose(post_anom, (1, 0, 2))[None, None])


def solution(mesh):
    in_specs = (
        P("gx", "gy", None, None, None),
        P("gx", "gy", None, None),
        P("gx", "gy", None, None, None),
        P("gx", "gy", None),
        P("gx", "gy", None),
        P("gx", "gy", None),
        P("gx", "gy", None),
        P("gx", "gy", None),
        P("gx", "gy", None),
    )
    out_specs = (P("gx", "gy", None, None), P("gx", "gy", None, None, None))
    return jax.shard_map(local, mesh=mesh, in_specs=in_specs, out_specs=out_specs, check_vma=False)
```

```python
import functools

import jax
import jax.numpy as jnp
import numpy as np
from jax import lax
from jax.experimental import pallas as pl
from jax.experimental.pallas import tpu as pltpu
from jax.sharding import PartitionSpec as P

AX = 8
AY = 16
OB = 32
NB = 2
RAD = 2
CODE = 64
LIMIT = 65400 * 1024

MESH = pl.DeviceIdType.MESH
OFFS = [(dx, dy) for dx in (-1, 0, 1) for dy in (-1, 0, 1)]
OTHERS = [i for i in range(9) if i != 4]


def taper_of(dx, dy):
    return max(1.0 - (dx * dx + dy * dy) / float(RAD * RAD), 0.0) ** 2


@functools.lru_cache
def tables():
    cells = AX * AY
    own = [(c // AY, c % AY) for c in range(cells)]
    halo = [
        (x, y)
        for x in range(-RAD, AX + RAD)
        for y in range(-RAD, AY + RAD)
        if not (0 <= x < AX and 0 <= y < AY)
    ]
    lanes = own + halo
    where = {xy: n for n, xy in enumerate(lanes)}
    code = np.full((8, 2 * cells), -1.0, np.float32)
    for n, (x, y) in enumerate(lanes):
        code[:, n] = (x + AX) * CODE + (y + AY)
    move = np.zeros((2 * cells, 2, 8, cells), np.float32)
    for n, (x, y) in enumerate(lanes):
        for d, i in enumerate(OTHERS):
            dx, dy = OFFS[i]
            src = where.get((x + dx, y + dy))
            if src is not None:
                move[src, n // cells, d, n % cells] = 1.0
    pick = np.zeros((8, cells, cells), np.float32)
    for n, (x, y) in enumerate(halo):
        i = (x // AX + 1) * 3 + (y // AY + 1)
        pick[OTHERS.index(i), (x % AX) * AY + (y % AY), n] = 1.0
    return code, move.reshape(2 * cells, 16 * cells), pick.reshape(8 * cells, cells)


def split_rows(block):
    high = block.astype(jnp.bfloat16).astype(jnp.float32)
    return jnp.concatenate([high, block - high], axis=0).astype(jnp.bfloat16)


def exchange_kernel(
    src_ref, order_ref, cell_ref, live_ref, value_ref, error_ref, ocean_ref, weights_ref, atm_ref,
    tiles_ref, metat_ref, fields_ref, fmean_ref,
    ocn, wts, meta, src, order_in, cell_in, live_in, value_in, error_in,
    own, blank, metat, held, fmean,
    local_sem, send_sem, recv_sem, out_sem,
):
    gx, gy = lax.axis_index("gx"), lax.axis_index("gy")
    nx, ny = lax.axis_size("gx"), lax.axis_size("gy")
    members = tiles_ref.shape[1]
    fields = atm_ref.shape[0]
    slots = order_in.shape[1]

    def has_x(dx):
        return (gx + dx >= 0) & (gx + dx < nx)

    def has_y(dy):
        return (gy + dy >= 0) & (gy + dy < ny)

    def there(i):
        return has_x(OFFS[i][0]) & has_y(OFFS[i][1])

    pairs = (
        (ocean_ref, ocn.at[4]), (order_ref, order_in), (cell_ref, cell_in), (live_ref, live_in),
        (value_ref, value_in), (error_ref, error_in), (src_ref, src), (weights_ref, wts),
        (atm_ref, held),
    )
    staged = [pltpu.make_async_copy(x, y, local_sem.at[n]) for n, (x, y) in enumerate(pairs)]
    for copy in staged:
        copy.start()

    blank[...] = jnp.zeros(blank.shape, jnp.float32)
    barrier = pltpu.get_barrier_semaphore()
    for i in OTHERS:
        dx, dy = OFFS[i]

        @pl.when(there(i))
        def _():
            pl.semaphore_signal(barrier, inc=1, device_id=(gx + dx, gy + dy), device_id_type=MESH)

    for i in OTHERS:

        @pl.when(jnp.logical_not(there(i)))
        def _():
            pltpu.make_async_copy(blank, tiles_ref.at[i], out_sem.at[i]).start()
            meta[i] = jnp.zeros(meta.shape[1:], jnp.float32)

    for n in range(9, meta.shape[0]):
        meta[n] = jnp.zeros(meta.shape[1:], jnp.float32)

    for copy in staged[1:6]:
        copy.wait()
    cell = cell_in[...]
    spot = ((cell // AY) * CODE + cell % AY).astype(jnp.float32)
    rows = jnp.concatenate(
        [
            spot, value_in[...], error_in[...], live_in[...].astype(jnp.float32),
            jnp.zeros((4, slots), jnp.float32),
        ],
        axis=0,
    )
    slot = lax.broadcasted_iota(jnp.int32, (slots, slots), 0)
    perm = jnp.where(order_in[...] == slot, 1.0, 0.0)
    rows = jnp.dot(rows, perm, precision=lax.Precision.HIGHEST, preferred_element_type=jnp.float32)
    meta[4] = jnp.concatenate([rows, jnp.zeros((8, meta.shape[2] - slots), jnp.float32)], axis=1)

    staged[0].wait()
    across = 1 + has_x(-1).astype(jnp.int32) + has_x(1).astype(jnp.int32)
    along = 1 + has_y(-1).astype(jnp.int32) + has_y(1).astype(jnp.int32)
    pl.semaphore_wait(barrier, across * along - 1)

    outer = lax.rem(gy, 2) * 2 - 1

    def ocean(source, target, n, dx, dy):
        return pltpu.make_async_remote_copy(
            src_ref=ocn.at[source],
            dst_ref=ocn.at[target],
            send_sem=send_sem.at[0, n],
            recv_sem=recv_sem.at[0, target],
            device_id=(gx + dx, gy + dy),
            device_id_type=MESH,
        )

    def arrive(at, dx, dy):
        ocean(at, at, 4, dx, dy).wait_recv()

    firsts = [
        (has_y(outer), ocean(4, 4 - outer, 1, 0, outer)),
        (has_x(-1), ocean(4, 7, 2, -1, 0)),
        (has_x(1), ocean(4, 1, 3, 1, 0)),
        (has_y(-outer), ocean(4, 4 + outer, 0, 0, -outer)),
    ]
    relays = [
        (has_y(outer) & has_x(dx), ocean(4 + outer, 4 - 3 * dx + outer, n, dx, 0))
        for dx, n in ((-1, 5), (1, 6))
    ]
    hands = [
        (dx, has_x(dx) & has_y(-outer), ocean(4 + 3 * dx, 4 + 3 * dx + outer, n, 0, -outer))
        for dx, n in ((-1, 7), (1, 8))
    ]

    def begin(cond, copy):
        @pl.when(cond)
        def _():
            copy.start()

    for cond, copy in firsts:
        begin(cond, copy)

    def remote(buf, kind, i):
        dx, dy = OFFS[i]
        return pltpu.make_async_remote_copy(
            src_ref=buf.at[4],
            dst_ref=buf.at[8 - i],
            send_sem=send_sem.at[kind, i],
            recv_sem=recv_sem.at[kind, 8 - i],
            device_id=(gx + dx, gy + dy),
            device_id_type=MESH,
        )

    def column(i):
        dx, dy = OFFS[i]
        return pltpu.make_async_remote_copy(
            src_ref=own,
            dst_ref=tiles_ref.at[8 - i],
            send_sem=send_sem.at[2, i],
            recv_sem=recv_sem.at[2, 8 - i],
            device_id=(gx + dx, gy + dy),
            device_id_type=MESH,
        )

    def send(buf, kind):
        for i in OTHERS:

            @pl.when(there(i))
            def _():
                remote(buf, kind, i).start()

    def receive(buf, kind):
        for i in OTHERS:

            @pl.when(there(i))
            def _():
                remote(buf, kind, 8 - i).wait_recv()

    def settle(buf, kind):
        for i in OTHERS:

            @pl.when(there(i))
            def _():
                remote(buf, kind, i).wait_send()

    send(meta, 1)

    staged[8].wait()
    for v in range(fields):
        block = held[v]
        mean = jnp.sum(block, axis=0, keepdims=True) / members
        fmean[v : v + 1, :] = mean
        held[v] = block - mean
    results = [
        pltpu.make_async_copy(held, fields_ref, local_sem.at[9]),
        pltpu.make_async_copy(fmean, fmean_ref, local_sem.at[10]),
        pltpu.make_async_copy(metat, metat_ref, local_sem.at[11]),
        pltpu.make_async_copy(own, tiles_ref.at[4], out_sem.at[4]),
    ]
    results[0].start()
    results[1].start()

    @pl.when(has_y(outer))
    def _():
        arrive(4 + outer, 0, outer)

    for cond, copy in relays:
        begin(cond, copy)
    for dx, cond, copy in hands:

        @pl.when(has_x(dx))
        def _():
            arrive(4 + 3 * dx, dx, 0)

        begin(cond, copy)

    receive(meta, 1)
    flat = meta[...].reshape(meta.shape[0] * meta.shape[1], meta.shape[2])
    metat[...] = flat.T
    results[2].start()
    staged[6].wait()
    staged[7].wait()

    @pl.when(has_y(-outer))
    def _():
        arrive(4 - outer, 0, -outer)

    for dx in (-1, 1):
        for dy in (outer, -outer):

            @pl.when(has_x(dx) & has_y(dy))
            def _():
                arrive(4 + 3 * dx + dy, dx, 0)

    total = jnp.zeros(tiles_ref.shape[1:], jnp.float32)
    for k in range(wts.shape[0]):
        source = src[0, k]
        position = (source // ny - gx + 1) * 3 + (source % ny - gy + 1)
        position = jnp.clip(position, 0, 8)
        total += jnp.dot(ocn[position], wts[k], preferred_element_type=jnp.float32)
    own[...] = total
    for i in OTHERS:

        @pl.when(there(i))
        def _():
            column(i).start()

    results[3].start()
    for cond, copy in firsts + relays + [hand[1:] for hand in hands]:

        @pl.when(cond)
        def _():
            copy.wait_send()

    settle(meta, 1)
    for copy in results:
        copy.wait()
    for i in OTHERS:

        @pl.when(jnp.logical_not(there(i)))
        def _():
            pltpu.make_async_copy(blank, tiles_ref.at[i], out_sem.at[i]).wait()

        @pl.when(there(i))
        def _():
            column(i).wait_send()
            column(8 - i).wait_recv()


def analysis_kernel(
    tiles_in, metat_in, fields_in, fmean_in, code_in, move_in, pick_in,
    mean_ref, anom_ref,
    tiles_ref, metat_ref, fmean_ref, code_ref, move_ref, pick_ref, held, shifted, local_sem, out_sem,
):
    fields, members, cells = fields_in.shape
    pairs = (
        (tiles_in, tiles_ref), (metat_in, metat_ref), (fmean_in, fmean_ref),
        (fields_in, held.at[0:fields]), (pick_in, pick_ref), (code_in, code_ref),
        (move_in, move_ref),
    )
    staged = [pltpu.make_async_copy(x, y, local_sem.at[n]) for n, (x, y) in enumerate(pairs)]
    for n in (0, 4, 1, 5, 6, 2, 3):
        staged[n].start()
    staged[0].wait()
    staged[4].wait()

    scale = 1.0 / (members - 1)
    beside = split_rows(jnp.concatenate([tiles_ref[i] for i in OTHERS], axis=1))
    halo = jnp.dot(beside, pick_ref[...], preferred_element_type=jnp.float32)
    grid = jnp.concatenate([tiles_ref[4], halo[:members] + halo[members:]], axis=1)
    gmean = jnp.sum(grid, axis=0, keepdims=True) / members
    grid = grid - gmean
    staged[1].wait()
    staged[5].wait()
    code = code_ref[0:1, :]

    for b in range(NB):
        last = b == NB - 1
        variance = jnp.sum(grid * grid, axis=0, keepdims=True) / (members - 1)
        gains = jnp.zeros((OB, 2 * cells), jnp.float32)
        sums = jnp.zeros((OB, 2 * cells), jnp.float32)
        weights = jnp.zeros((OB, 2 * cells), jnp.float32)
        for i in range(9):
            dx, dy = OFFS[i]
            column = metat_ref[b * OB : (b + 1) * OB, 8 * i : 8 * i + 4]
            spot = column[:, 0:1] + float((AX * dx + AX) * CODE + AY * dy + AY)
            error = column[:, 2:3]
            live = column[:, 3:4]
            denom = variance + (error + (1.0 - live))
            weighting = live / denom
            damping = 1.0 / (1.0 + jnp.sqrt(error / denom))
            hit = spot == code
            weighting = jnp.where(hit, weighting, 0.0)
            weights = weights + weighting
            gains = gains + weighting * damping
            sums = sums + weighting * column[:, 1:2]
        alpha = jnp.sum(gains, axis=0, keepdims=True)
        beta = jnp.sum(sums, axis=0, keepdims=True) - gmean * jnp.sum(weights, axis=0, keepdims=True)
        extra = jnp.concatenate([alpha, beta, jnp.zeros((6, 2 * cells), jnp.float32)], axis=0)
        if b == 0:
            staged[6].wait()
        left = split_rows(jnp.concatenate([grid, extra], axis=0))
        width = (8 if last else 16) * cells
        moved = jnp.dot(left, move_ref[:, :width], preferred_element_type=jnp.float32)
        rows = members + 8
        shifted[:, :width] = moved[:rows] + moved[rows:]

        def step(block, part, center, alpha, beta):
            total = jnp.zeros_like(block)
            mean = jnp.zeros((1, cells), jnp.float32)
            for d in range(9):
                if d == 8:
                    source, a, m = center, alpha * scale, beta * scale
                else:
                    dx, dy = OFFS[OTHERS[d]]
                    weight = scale * taper_of(dx, dy)
                    at = (part * 8 + d) * cells
                    source = shifted[:members, at : at + cells]
                    a = shifted[members : members + 1, at : at + cells] * weight
                    m = shifted[members + 1 : members + 2, at : at + cells] * weight
                cov = jnp.sum(block * source, axis=0, keepdims=True)
                mean = mean + cov * m
                total = total + source * (cov * a)
            return block - total, mean

        own = grid[:, :cells]
        held[fields] = own
        if b == 0:
            staged[2].wait()
            staged[3].wait()
        own_args = (alpha[:, :cells], beta[:, :cells])

        def one_field(v, carry, own_args=own_args, last=last, b=b, step=step):
            block, mean = step(held[v], 0, held[fields], *own_args)
            held[v] = block
            before = fmean_ref[pl.ds(v, 1), :] if b == 0 else mean_ref[v]
            mean_ref[v] = before + mean
            if last:
                pltpu.make_async_copy(held.at[v], anom_ref.at[v], out_sem.at[v]).start()
            return carry

        lax.fori_loop(0, fields, one_field, 0)
        block, mean = step(own, 0, own, *own_args)
        if last:
            held[fields] = block
            mean_ref[fields] = gmean[:, :cells] + mean
            pltpu.make_async_copy(
                held.at[fields], anom_ref.at[fields], out_sem.at[fields]
            ).start()
            for v in range(fields + 1):
                pltpu.make_async_copy(held.at[v], anom_ref.at[v], out_sem.at[v]).wait()
        else:
            outer = grid[:, cells:]
            far, far_mean = step(outer, 1, outer, alpha[:, cells:], beta[:, cells:])
            grid = jnp.concatenate([block, far], axis=1)
            gmean = gmean + jnp.concatenate([mean, far_mean], axis=1)


def local(
    atm_members, ocean_members, remap_weights, pair_src, obs_cell, obs_value, obs_error,
    obs_live, obs_order,
):
    members, fields, cells = atm_members.shape[2:]
    slots = obs_cell.shape[2]
    sources, depth = remap_weights.shape[2:4]
    vmem = pl.BlockSpec(memory_space=pltpu.VMEM)
    anywhere = pl.BlockSpec(memory_space=pl.ANY)
    code, move, pick = tables()
    results = (
        jax.ShapeDtypeStruct((9, members, cells), jnp.float32),
        jax.ShapeDtypeStruct((128, 128), jnp.float32),
        jax.ShapeDtypeStruct((fields, members, cells), jnp.float32),
        jax.ShapeDtypeStruct((fields, cells), jnp.float32),
    )
    state = pl.pallas_call(
        exchange_kernel,
        out_shape=results,
        in_specs=[anywhere] * 9,
        out_specs=(anywhere,) * 4,
        scratch_shapes=[
            pltpu.VMEM((9, members, depth), jnp.bfloat16),
            pltpu.VMEM((sources, depth, cells), jnp.bfloat16),
            pltpu.VMEM((16, 8, 128), jnp.float32),
            pltpu.SMEM((1, sources), jnp.int32),
            pltpu.VMEM((1, slots), jnp.int32),
            pltpu.VMEM((1, slots), jnp.int32),
            pltpu.VMEM((1, slots), jnp.int32),
            pltpu.VMEM((1, slots), jnp.float32),
            pltpu.VMEM((1, slots), jnp.float32),
            pltpu.VMEM((members, cells), jnp.float32),
            pltpu.VMEM((members, cells), jnp.float32),
            pltpu.VMEM((128, 128), jnp.float32),
            pltpu.VMEM((fields, members, cells), jnp.float32),
            pltpu.VMEM((fields, cells), jnp.float32),
            pltpu.SemaphoreType.DMA((12,)),
            pltpu.SemaphoreType.DMA((3, 9)),
            pltpu.SemaphoreType.DMA((3, 9)),
            pltpu.SemaphoreType.DMA((9,)),
        ],
        compiler_params=pltpu.CompilerParams(
            collective_id=0, has_side_effects=True, vmem_limit_bytes=LIMIT
        ),
        name="exchange",
    )(
        pair_src[0], obs_order[0], obs_cell[0], obs_live[0], obs_value[0], obs_error[0],
        ocean_members[0, 0], remap_weights[0, 0], jnp.transpose(atm_members[0, 0], (1, 0, 2)),
    )
    post_mean, post_anom = pl.pallas_call(
        analysis_kernel,
        out_shape=(
            jax.ShapeDtypeStruct((fields + 1, 1, cells), jnp.float32),
            jax.ShapeDtypeStruct((fields + 1, members, cells), jnp.float32),
        ),
        in_specs=[anywhere] * 7,
        out_specs=(vmem, anywhere),
        scratch_shapes=[
            *(pltpu.VMEM(r.shape, jnp.float32) for r in (results[0], results[1], results[3])),
            pltpu.VMEM(code.shape, jnp.float32),
            pltpu.VMEM(move.shape, jnp.bfloat16),
            pltpu.VMEM(pick.shape, jnp.bfloat16),
            pltpu.VMEM((fields + 1, members, cells), jnp.float32),
            pltpu.VMEM((members + 8, 16 * cells), jnp.float32),
            pltpu.SemaphoreType.DMA((7,)),
            pltpu.SemaphoreType.DMA((fields + 1,)),
        ],
        compiler_params=pltpu.CompilerParams(vmem_limit_bytes=LIMIT),
        name="analysis",
    )(*state, jnp.asarray(code), jnp.asarray(move, jnp.bfloat16), jnp.asarray(pick, jnp.bfloat16))
    return (post_mean.reshape(1, 1, fields + 1, cells), jnp.transpose(post_anom, (1, 0, 2))[None, None])


def solution(mesh):
    in_specs = (
        P("gx", "gy", None, None, None),
        P("gx", "gy", None, None),
        P("gx", "gy", None, None, None),
        P("gx", "gy", None),
        P("gx", "gy", None),
        P("gx", "gy", None),
        P("gx", "gy", None),
        P("gx", "gy", None),
        P("gx", "gy", None),
    )
    out_specs = (P("gx", "gy", None, None), P("gx", "gy", None, None, None))
    return jax.shard_map(local, mesh=mesh, in_specs=in_specs, out_specs=out_specs, check_vma=False)
```

```python
import functools

import jax
import jax.numpy as jnp
import numpy as np
from jax import lax
from jax.experimental import pallas as pl
from jax.experimental.pallas import tpu as pltpu
from jax.sharding import PartitionSpec as P

AX = 8
AY = 16
OB = 32
NB = 2
RAD = 2
CODE = 64
LIMIT = 65400 * 1024

MESH = pl.DeviceIdType.MESH
OFFS = [(dx, dy) for dx in (-1, 0, 1) for dy in (-1, 0, 1)]
OTHERS = [i for i in range(9) if i != 4]


def taper_of(dx, dy):
    return max(1.0 - (dx * dx + dy * dy) / float(RAD * RAD), 0.0) ** 2


@functools.lru_cache
def tables():
    cells = AX * AY
    own = [(c // AY, c % AY) for c in range(cells)]
    halo = [
        (x, y)
        for x in range(-RAD, AX + RAD)
        for y in range(-RAD, AY + RAD)
        if not (0 <= x < AX and 0 <= y < AY)
    ]
    lanes = own + halo
    where = {xy: n for n, xy in enumerate(lanes)}
    code = np.full((8, 2 * cells), -1.0, np.float32)
    for n, (x, y) in enumerate(lanes):
        code[:, n] = (x + AX) * CODE + (y + AY)
    move = np.zeros((2 * cells, 2, 8, cells), np.float32)
    for n, (x, y) in enumerate(lanes):
        for d, i in enumerate(OTHERS):
            dx, dy = OFFS[i]
            src = where.get((x + dx, y + dy))
            if src is not None:
                move[src, n // cells, d, n % cells] = 1.0
    pick = np.zeros((8, cells, cells), np.float32)
    for n, (x, y) in enumerate(halo):
        i = (x // AX + 1) * 3 + (y // AY + 1)
        pick[OTHERS.index(i), (x % AX) * AY + (y % AY), n] = 1.0
    return code, move.reshape(2 * cells, 16 * cells), pick.reshape(8 * cells, cells)


def split_rows(block):
    high = block.astype(jnp.bfloat16).astype(jnp.float32)
    return jnp.concatenate([high, block - high], axis=0).astype(jnp.bfloat16)


def exchange_kernel(
    src_ref, order_ref, cell_ref, live_ref, value_ref, error_ref, ocean_ref, weights_ref, atm_ref,
    tiles_ref, metat_ref, fields_ref, fmean_ref,
    ocn, wts, meta, src, order_in, cell_in, live_in, value_in, error_in,
    own, blank, metat, held, fmean,
    local_sem, send_sem, recv_sem, out_sem,
):
    gx, gy = lax.axis_index("gx"), lax.axis_index("gy")
    nx, ny = lax.axis_size("gx"), lax.axis_size("gy")
    members = tiles_ref.shape[1]
    fields = atm_ref.shape[0]
    slots = order_in.shape[1]

    def has_x(dx):
        return (gx + dx >= 0) & (gx + dx < nx)

    def has_y(dy):
        return (gy + dy >= 0) & (gy + dy < ny)

    def there(i):
        return has_x(OFFS[i][0]) & has_y(OFFS[i][1])

    pairs = (
        (ocean_ref, ocn.at[4]), (order_ref, order_in), (cell_ref, cell_in), (live_ref, live_in),
        (value_ref, value_in), (error_ref, error_in), (src_ref, src), (weights_ref, wts),
        (atm_ref, held),
    )
    staged = [pltpu.make_async_copy(x, y, local_sem.at[n]) for n, (x, y) in enumerate(pairs)]
    for copy in staged:
        copy.start()

    blank[...] = jnp.zeros(blank.shape, jnp.float32)
    barrier = pltpu.get_barrier_semaphore()
    for i in OTHERS:
        dx, dy = OFFS[i]

        @pl.when(there(i))
        def _():
            pl.semaphore_signal(barrier, inc=1, device_id=(gx + dx, gy + dy), device_id_type=MESH)

    for i in OTHERS:

        @pl.when(jnp.logical_not(there(i)))
        def _():
            pltpu.make_async_copy(blank, tiles_ref.at[i], out_sem.at[i]).start()
            meta[i] = jnp.zeros(meta.shape[1:], jnp.float32)

    for n in range(9, meta.shape[0]):
        meta[n] = jnp.zeros(meta.shape[1:], jnp.float32)

    for copy in staged[1:6]:
        copy.wait()
    cell = cell_in[...]
    spot = ((cell // AY) * CODE + cell % AY).astype(jnp.float32)
    rows = jnp.concatenate(
        [
            spot, value_in[...], error_in[...], live_in[...].astype(jnp.float32),
            jnp.zeros((4, slots), jnp.float32),
        ],
        axis=0,
    )
    slot = lax.broadcasted_iota(jnp.int32, (slots, slots), 0)
    perm = jnp.where(order_in[...] == slot, 1.0, 0.0)
    rows = jnp.dot(rows, perm, precision=lax.Precision.HIGHEST, preferred_element_type=jnp.float32)
    meta[4] = jnp.concatenate([rows, jnp.zeros((8, meta.shape[2] - slots), jnp.float32)], axis=1)

    staged[0].wait()
    across = 1 + has_x(-1).astype(jnp.int32) + has_x(1).astype(jnp.int32)
    along = 1 + has_y(-1).astype(jnp.int32) + has_y(1).astype(jnp.int32)
    pl.semaphore_wait(barrier, across * along - 1)

    outer = lax.rem(gy, 2) * 2 - 1

    first = (members // 2 + 15) // 16 * 16
    parts = ((0, 0, first), (3, first, members - first))

    def ocean(part, source, target, n, dx, dy):
        kind, low, size = part
        return pltpu.make_async_remote_copy(
            src_ref=ocn.at[source, pl.ds(low, size)],
            dst_ref=ocn.at[target, pl.ds(low, size)],
            send_sem=send_sem.at[kind, n],
            recv_sem=recv_sem.at[kind, target],
            device_id=(gx + dx, gy + dy),
            device_id_type=MESH,
        )

    def arrive(part, at, dx, dy):
        ocean(part, at, at, 4, dx, dy).wait_recv()

    firsts = [
        (cond, ocean(part, 4, target, n, dx, dy))
        for part in parts
        for cond, target, n, dx, dy in (
            (has_y(outer), 4 - outer, 1, 0, outer),
            (has_x(-1), 7, 2, -1, 0),
            (has_x(1), 1, 3, 1, 0),
            (has_y(-outer), 4 + outer, 0, 0, -outer),
        )
    ]
    relays = [
        (has_y(outer) & has_x(dx), ocean(part, 4 + outer, 4 - 3 * dx + outer, n, dx, 0))
        for part in parts
        for dx, n in ((-1, 5), (1, 6))
    ]
    hands = [
        (
            part, dx, has_x(dx) & has_y(-outer),
            ocean(part, 4 + 3 * dx, 4 + 3 * dx + outer, n, 0, -outer),
        )
        for part in parts
        for dx, n in ((-1, 7), (1, 8))
    ]

    def begin(cond, copy):
        @pl.when(cond)
        def _():
            copy.start()

    for cond, copy in firsts:
        begin(cond, copy)

    def remote(buf, kind, i):
        dx, dy = OFFS[i]
        return pltpu.make_async_remote_copy(
            src_ref=buf.at[4],
            dst_ref=buf.at[8 - i],
            send_sem=send_sem.at[kind, i],
            recv_sem=recv_sem.at[kind, 8 - i],
            device_id=(gx + dx, gy + dy),
            device_id_type=MESH,
        )

    def column(i):
        dx, dy = OFFS[i]
        return pltpu.make_async_remote_copy(
            src_ref=own,
            dst_ref=tiles_ref.at[8 - i],
            send_sem=send_sem.at[2, i],
            recv_sem=recv_sem.at[2, 8 - i],
            device_id=(gx + dx, gy + dy),
            device_id_type=MESH,
        )

    def send(buf, kind):
        for i in OTHERS:

            @pl.when(there(i))
            def _():
                remote(buf, kind, i).start()

    def receive(buf, kind):
        for i in OTHERS:

            @pl.when(there(i))
            def _():
                remote(buf, kind, 8 - i).wait_recv()

    def settle(buf, kind):
        for i in OTHERS:

            @pl.when(there(i))
            def _():
                remote(buf, kind, i).wait_send()

    send(meta, 1)

    staged[8].wait()
    for v in range(fields):
        block = held[v]
        mean = jnp.sum(block, axis=0, keepdims=True) / members
        fmean[v : v + 1, :] = mean
        held[v] = block - mean
    results = [
        pltpu.make_async_copy(held, fields_ref, local_sem.at[9]),
        pltpu.make_async_copy(fmean, fmean_ref, local_sem.at[10]),
        pltpu.make_async_copy(metat, metat_ref, local_sem.at[11]),
        pltpu.make_async_copy(own, tiles_ref.at[4], out_sem.at[4]),
    ]
    results[0].start()
    results[1].start()

    for at, part in enumerate(parts):

        @pl.when(has_y(outer))
        def _():
            arrive(part, 4 + outer, 0, outer)

        for cond, copy in relays[2 * at : 2 * at + 2]:
            begin(cond, copy)
    for part, dx, cond, copy in hands:

        @pl.when(has_x(dx))
        def _():
            arrive(part, 4 + 3 * dx, dx, 0)

        begin(cond, copy)

    receive(meta, 1)
    flat = meta[...].reshape(meta.shape[0] * meta.shape[1], meta.shape[2])
    metat[...] = flat.T
    results[2].start()
    staged[6].wait()
    staged[7].wait()

    for part in parts:

        @pl.when(has_y(-outer))
        def _():
            arrive(part, 4 - outer, 0, -outer)

        for dx in (-1, 1):
            for dy in (outer, -outer):

                @pl.when(has_x(dx) & has_y(dy))
                def _():
                    arrive(part, 4 + 3 * dx + dy, dx, 0)

    total = jnp.zeros(tiles_ref.shape[1:], jnp.float32)
    for k in range(wts.shape[0]):
        source = src[0, k]
        position = (source // ny - gx + 1) * 3 + (source % ny - gy + 1)
        position = jnp.clip(position, 0, 8)
        total += jnp.dot(ocn[position], wts[k], preferred_element_type=jnp.float32)
    own[...] = total
    for i in OTHERS:

        @pl.when(there(i))
        def _():
            column(i).start()

    results[3].start()
    for cond, copy in firsts + relays + [hand[2:] for hand in hands]:

        @pl.when(cond)
        def _():
            copy.wait_send()

    settle(meta, 1)
    for copy in results:
        copy.wait()
    for i in OTHERS:

        @pl.when(jnp.logical_not(there(i)))
        def _():
            pltpu.make_async_copy(blank, tiles_ref.at[i], out_sem.at[i]).wait()

        @pl.when(there(i))
        def _():
            column(i).wait_send()
            column(8 - i).wait_recv()


def analysis_kernel(
    tiles_in, metat_in, fields_in, fmean_in, code_in, move_in, pick_in,
    mean_ref, anom_ref,
    tiles_ref, metat_ref, fmean_ref, code_ref, move_ref, pick_ref, held, shifted, local_sem, out_sem,
):
    fields, members, cells = fields_in.shape
    pairs = (
        (tiles_in, tiles_ref), (metat_in, metat_ref), (fmean_in, fmean_ref),
        (fields_in, held.at[0:fields]), (pick_in, pick_ref), (code_in, code_ref),
        (move_in, move_ref),
    )
    staged = [pltpu.make_async_copy(x, y, local_sem.at[n]) for n, (x, y) in enumerate(pairs)]
    for n in (0, 4, 1, 5, 6, 2, 3):
        staged[n].start()
    staged[0].wait()
    staged[4].wait()

    scale = 1.0 / (members - 1)
    beside = split_rows(jnp.concatenate([tiles_ref[i] for i in OTHERS], axis=1))
    halo = jnp.dot(beside, pick_ref[...], preferred_element_type=jnp.float32)
    grid = jnp.concatenate([tiles_ref[4], halo[:members] + halo[members:]], axis=1)
    gmean = jnp.sum(grid, axis=0, keepdims=True) / members
    grid = grid - gmean
    staged[1].wait()
    staged[5].wait()
    code = code_ref[0:1, :]

    for b in range(NB):
        last = b == NB - 1
        variance = jnp.sum(grid * grid, axis=0, keepdims=True) / (members - 1)
        gains = jnp.zeros((OB, 2 * cells), jnp.float32)
        sums = jnp.zeros((OB, 2 * cells), jnp.float32)
        weights = jnp.zeros((OB, 2 * cells), jnp.float32)
        for i in range(9):
            dx, dy = OFFS[i]
            column = metat_ref[b * OB : (b + 1) * OB, 8 * i : 8 * i + 4]
            spot = column[:, 0:1] + float((AX * dx + AX) * CODE + AY * dy + AY)
            error = column[:, 2:3]
            live = column[:, 3:4]
            denom = variance + (error + (1.0 - live))
            weighting = live / denom
            damping = 1.0 / (1.0 + jnp.sqrt(error / denom))
            hit = spot == code
            weighting = jnp.where(hit, weighting, 0.0)
            weights = weights + weighting
            gains = gains + weighting * damping
            sums = sums + weighting * column[:, 1:2]
        alpha = jnp.sum(gains, axis=0, keepdims=True)
        beta = jnp.sum(sums, axis=0, keepdims=True) - gmean * jnp.sum(weights, axis=0, keepdims=True)
        extra = jnp.concatenate([alpha, beta, jnp.zeros((6, 2 * cells), jnp.float32)], axis=0)
        if b == 0:
            staged[6].wait()
        left = split_rows(jnp.concatenate([grid, extra], axis=0))
        width = (8 if last else 16) * cells
        moved = jnp.dot(left, move_ref[:, :width], preferred_element_type=jnp.float32)
        rows = members + 8
        shifted[:, :width] = moved[:rows] + moved[rows:]

        def step(block, part, center, alpha, beta):
            total = jnp.zeros_like(block)
            mean = jnp.zeros((1, cells), jnp.float32)
            for d in range(9):
                if d == 8:
                    source, a, m = center, alpha * scale, beta * scale
                else:
                    dx, dy = OFFS[OTHERS[d]]
                    weight = scale * taper_of(dx, dy)
                    at = (part * 8 + d) * cells
                    source = shifted[:members, at : at + cells]
                    a = shifted[members : members + 1, at : at + cells] * weight
                    m = shifted[members + 1 : members + 2, at : at + cells] * weight
                cov = jnp.sum(block * source, axis=0, keepdims=True)
                mean = mean + cov * m
                total = total + source * (cov * a)
            return block - total, mean

        own = grid[:, :cells]
        held[fields] = own
        if b == 0:
            staged[2].wait()
            staged[3].wait()
        own_args = (alpha[:, :cells], beta[:, :cells])

        def one_field(v, carry, own_args=own_args, last=last, b=b, step=step):
            block, mean = step(held[v], 0, held[fields], *own_args)
            held[v] = block
            before = fmean_ref[pl.ds(v, 1), :] if b == 0 else mean_ref[v]
            mean_ref[v] = before + mean
            if last:
                pltpu.make_async_copy(held.at[v], anom_ref.at[v], out_sem.at[v]).start()
            return carry

        lax.fori_loop(0, fields, one_field, 0)
        block, mean = step(own, 0, own, *own_args)
        if last:
            held[fields] = block
            mean_ref[fields] = gmean[:, :cells] + mean
            pltpu.make_async_copy(
                held.at[fields], anom_ref.at[fields], out_sem.at[fields]
            ).start()
            for v in range(fields + 1):
                pltpu.make_async_copy(held.at[v], anom_ref.at[v], out_sem.at[v]).wait()
        else:
            outer = grid[:, cells:]
            far, far_mean = step(outer, 1, outer, alpha[:, cells:], beta[:, cells:])
            grid = jnp.concatenate([block, far], axis=1)
            gmean = gmean + jnp.concatenate([mean, far_mean], axis=1)


def local(
    atm_members, ocean_members, remap_weights, pair_src, obs_cell, obs_value, obs_error,
    obs_live, obs_order,
):
    members, fields, cells = atm_members.shape[2:]
    slots = obs_cell.shape[2]
    sources, depth = remap_weights.shape[2:4]
    vmem = pl.BlockSpec(memory_space=pltpu.VMEM)
    anywhere = pl.BlockSpec(memory_space=pl.ANY)
    code, move, pick = tables()
    results = (
        jax.ShapeDtypeStruct((9, members, cells), jnp.float32),
        jax.ShapeDtypeStruct((128, 128), jnp.float32),
        jax.ShapeDtypeStruct((fields, members, cells), jnp.float32),
        jax.ShapeDtypeStruct((fields, cells), jnp.float32),
    )
    state = pl.pallas_call(
        exchange_kernel,
        out_shape=results,
        in_specs=[anywhere] * 9,
        out_specs=(anywhere,) * 4,
        scratch_shapes=[
            pltpu.VMEM((9, members, depth), jnp.bfloat16),
            pltpu.VMEM((sources, depth, cells), jnp.bfloat16),
            pltpu.VMEM((16, 8, 128), jnp.float32),
            pltpu.SMEM((1, sources), jnp.int32),
            pltpu.VMEM((1, slots), jnp.int32),
            pltpu.VMEM((1, slots), jnp.int32),
            pltpu.VMEM((1, slots), jnp.int32),
            pltpu.VMEM((1, slots), jnp.float32),
            pltpu.VMEM((1, slots), jnp.float32),
            pltpu.VMEM((members, cells), jnp.float32),
            pltpu.VMEM((members, cells), jnp.float32),
            pltpu.VMEM((128, 128), jnp.float32),
            pltpu.VMEM((fields, members, cells), jnp.float32),
            pltpu.VMEM((fields, cells), jnp.float32),
            pltpu.SemaphoreType.DMA((12,)),
            pltpu.SemaphoreType.DMA((4, 9)),
            pltpu.SemaphoreType.DMA((4, 9)),
            pltpu.SemaphoreType.DMA((9,)),
        ],
        compiler_params=pltpu.CompilerParams(
            collective_id=0, has_side_effects=True, vmem_limit_bytes=LIMIT
        ),
        name="exchange",
    )(
        pair_src[0], obs_order[0], obs_cell[0], obs_live[0], obs_value[0], obs_error[0],
        ocean_members[0, 0], remap_weights[0, 0], jnp.transpose(atm_members[0, 0], (1, 0, 2)),
    )
    post_mean, post_anom = pl.pallas_call(
        analysis_kernel,
        out_shape=(
            jax.ShapeDtypeStruct((fields + 1, 1, cells), jnp.float32),
            jax.ShapeDtypeStruct((fields + 1, members, cells), jnp.float32),
        ),
        in_specs=[anywhere] * 7,
        out_specs=(vmem, anywhere),
        scratch_shapes=[
            *(pltpu.VMEM(r.shape, jnp.float32) for r in (results[0], results[1], results[3])),
            pltpu.VMEM(code.shape, jnp.float32),
            pltpu.VMEM(move.shape, jnp.bfloat16),
            pltpu.VMEM(pick.shape, jnp.bfloat16),
            pltpu.VMEM((fields + 1, members, cells), jnp.float32),
            pltpu.VMEM((members + 8, 16 * cells), jnp.float32),
            pltpu.SemaphoreType.DMA((7,)),
            pltpu.SemaphoreType.DMA((fields + 1,)),
        ],
        compiler_params=pltpu.CompilerParams(vmem_limit_bytes=LIMIT),
        name="analysis",
    )(*state, jnp.asarray(code), jnp.asarray(move, jnp.bfloat16), jnp.asarray(pick, jnp.bfloat16))
    return (post_mean.reshape(1, 1, fields + 1, cells), jnp.transpose(post_anom, (1, 0, 2))[None, None])


def solution(mesh):
    in_specs = (
        P("gx", "gy", None, None, None),
        P("gx", "gy", None, None),
        P("gx", "gy", None, None, None),
        P("gx", "gy", None),
        P("gx", "gy", None),
        P("gx", "gy", None),
        P("gx", "gy", None),
        P("gx", "gy", None),
        P("gx", "gy", None),
    )
    out_specs = (P("gx", "gy", None, None), P("gx", "gy", None, None, None))
    return jax.shard_map(local, mesh=mesh, in_specs=in_specs, out_specs=out_specs, check_vma=False)
```
